256 devices in a mesh: beam: 4 (over y, x), fft: 64 (over z, core).
Axes of the slice: x: 2, y: 2, z: 32, core: 2. Of those that a mesh axis runs over, the one named last changes fastest.
The devices are a block of a 4x8x32 slice.
Arguments:
- baseband: bfloat16 [8, 33554432], P('beam', 'fft'), parts along dimension 0, may hold values from -6 to 6
- spectrum_in: bfloat16 [8, 4096, 8192], P('beam', 'fft'), parts along dimension 0, may hold values from -6 to 6
- dm_index: int32 [1], replicated, may hold values from 0 to 63
Outputs:
- spectrum_out: bfloat16 [8, 4096, 8192], P('beam', 'fft'), parts along dimension 0
- smoothed: float32 [4, 2097152], P('beam', 'fft'), parts along dimension 0
The draws below stay inside these ranges and needn't reach their ends.
There are 4 independent parts, one for each index of `beam`. The reference program is written for one: setup_inputs(seed, part) draws one part's arguments, and reference() takes and returns one part's arrays. A program takes and returns all parts, laid end to end along the dimension named above; an argument that names none is the same for every part. Nothing has to cross between parts.
Inputs may be any that keep to these rules, and one draw needn't show every extreme that they name: `dm_index`: indices into the grid of 64 trial dispersion measures.
All inputs are finite; a program needn't handle non-finite values.
Results may differ from the reference program's by a relative error of at most 0.0019.
The reference program's roundings to bfloat16 on the way count: a program that leaves them out, or rounds other values in their place, can miss the bound.
Values may be sent and summed in bfloat16 or wider, within the bound.
A program may use at most 64 MiB of HBM per device.

```python
import math
import jax
import jax.numpy as jnp
from jax import lax

ROWS_OUTER = 32
ROWS_INNER = 128
COLS_OUTER = 64
COLS_INNER = 128
ROW_LENGTH = 4096
COLUMN_LENGTH = 8192
SEGMENT_SAMPLES = 33554432
TRIALS = 1
DM_GRID = 64
DECIMATE_FACTOR = 16
HALF_WIDTH = 16


def block_scale(own_key, dims, pieces, smallest, largest):
    factor_of = 1.0
    for dim, parts in pieces:
        heights = jax.random.uniform(jax.random.fold_in(jax.random.fold_in(own_key, 6), dim), (parts,), jnp.float32, smallest / len(pieces), largest / len(pieces))
        factor_of = factor_of * jnp.repeat(jnp.exp(heights), dims[dim] // parts).reshape((-1,) + (1,) * (len(dims) - 1 - dim))
    return factor_of


def gaussian(rng, shape, scale, reach, split=(), kind=jnp.bfloat16):
    array = scale * jax.random.normal(rng, shape, jnp.float32)
    if split:
        array = array * block_scale(rng, shape, split, -0.22, 0.18)
    return jnp.clip(array, -reach, reach).astype(kind)


def setup_inputs(seed: int = 0, part: int = 0) -> dict:
    streams_of = jax.random.split(jax.random.key(seed), 4)
    own_keys = jax.random.split(jax.random.fold_in(streams_of[3], part), 4)
    baseband = gaussian(own_keys[0], (2, SEGMENT_SAMPLES), 1.0, 6.0, ((1, 64),))
    spectrum_in = gaussian(own_keys[1], (2, ROW_LENGTH, COLUMN_LENGTH), 1.0, 6.0, ((1, 64),))
    dm_index = jax.random.randint(streams_of[2], (TRIALS,), 0, DM_GRID).astype(jnp.int32)
    return dict(baseband=baseband, spectrum_in=spectrum_in, dm_index=dm_index)


def dft_table(length, direction):
    positions = jnp.arange(length, dtype=jnp.int32)
    product = jnp.remainder(positions[:, None] * positions[None, :], length)
    radians = direction * 2.0 * math.pi / length * product.astype(jnp.float32)
    norm_scale = 1.0 / math.sqrt(length)
    cosine = jnp.cos(radians) * norm_scale
    sine_part = jnp.sin(radians) * norm_scale
    return jnp.stack([jnp.stack([cosine, sine_part]), jnp.stack([-sine_part, cosine])]).astype(jnp.bfloat16)

def radians_of(numer, modulus, direction):
    return direction * 2.0 * math.pi / modulus * jnp.remainder(numer, modulus).astype(jnp.float32)

def chirp_radians(freq_row, col_outer, col_inner, grid_steps):
    col_freq = col_outer + COLS_OUTER * col_inner
    whole_mod = 4.0 * DM_GRID * ROW_LENGTH * COLUMN_LENGTH
    cross_mod = 2 * DM_GRID * COLUMN_LENGTH
    square_mod = 4 * DM_GRID * COLUMN_LENGTH
    grid_float = grid_steps.astype(jnp.float32)
    row_square = (freq_row * freq_row).astype(jnp.float32)
    term_rows = grid_float[:, None, None, None] * row_square[None, :, None, None] / whole_mod
    cross = jnp.remainder(freq_row[:, None, None] * col_freq[None], cross_mod)
    cross = jnp.remainder(grid_steps[:, None, None, None] * cross[None], cross_mod)
    square = jnp.remainder(col_freq * col_freq, square_mod)
    square = jnp.remainder(grid_steps[:, None, None] * square[None], square_mod)
    high_part = square // 512
    low_part = square % 512
    square = jnp.remainder(jnp.remainder(ROW_LENGTH * high_part, square_mod) * 512 + ROW_LENGTH * low_part, square_mod)
    turns = term_rows + cross.astype(jnp.float32) / cross_mod + square[:, None].astype(jnp.float32) / square_mod
    return 2.0 * math.pi * turns

def rotate(values, radians):
    cosine = jnp.cos(radians)
    sine_part = jnp.sin(radians)
    real_part = values[:, 0] * cosine - values[:, 1] * sine_part
    imag_part = values[:, 0] * sine_part + values[:, 1] * cosine
    return jnp.stack([real_part, imag_part], axis=1).astype(jnp.bfloat16)

def dft_section(values, einsum_form, length, direction, radians):
    mixed_sum = jnp.einsum(einsum_form, values.astype(jnp.float32), dft_table(length, direction).astype(jnp.float32), precision=lax.Precision.HIGHEST)
    if radians is None:
        return mixed_sum.astype(jnp.bfloat16)
    return rotate(mixed_sum, radians)

def row_frequency(row_pos):
    return row_pos // ROWS_INNER + ROWS_OUTER * (row_pos % ROWS_INNER)

def forward_spectrum(baseband):
    values = baseband.reshape(1, 2, ROWS_OUTER, ROWS_INNER, COLUMN_LENGTH)
    outer_pos = jnp.arange(ROWS_OUTER, dtype=jnp.int32)[:, None]
    inner_pos = jnp.arange(ROWS_INNER, dtype=jnp.int32)[None, :]
    values = dft_section(values, 'dixyb,ioxk->dokyb', ROWS_OUTER, -1, radians_of(outer_pos * inner_pos, ROW_LENGTH, -1)[:, :, None])
    freq_row = outer_pos + ROWS_OUTER * inner_pos
    col_pos = jnp.arange(COLUMN_LENGTH, dtype=jnp.int32)
    values = dft_section(values, 'dikyb,ioyq->dokqb', ROWS_INNER, -1, radians_of(freq_row[:, :, None] * col_pos[None, None, :], SEGMENT_SAMPLES, -1))
    values = values.reshape(1, 2, ROW_LENGTH, COLS_OUTER, COLS_INNER)
    col_outer = jnp.arange(COLS_OUTER, dtype=jnp.int32)[:, None]
    col_inner = jnp.arange(COLS_INNER, dtype=jnp.int32)[None, :]
    values = dft_section(values, 'dimxy,ioxj->domjy', COLS_OUTER, -1, radians_of(col_outer * col_inner, COLUMN_LENGTH, -1))
    values = dft_section(values, 'dimjy,ioyq->domjq', COLS_INNER, -1, None)
    return values[0].reshape(2, ROW_LENGTH, COLUMN_LENGTH)

def dedisperse(spectrum, grid_steps):
    trial_total = grid_steps.shape[0]
    row_pos = jnp.arange(ROW_LENGTH, dtype=jnp.int32)
    freq_row = row_frequency(row_pos)
    col_outer = jnp.arange(COLS_OUTER, dtype=jnp.int32)[:, None]
    col_inner = jnp.arange(COLS_INNER, dtype=jnp.int32)[None, :]
    values = rotate(spectrum.astype(jnp.float32).reshape(1, 2, ROW_LENGTH, COLS_OUTER, COLS_INNER), chirp_radians(freq_row, col_outer, col_inner, grid_steps))
    values = dft_section(values, 'dimjq,ioqy->domjy', COLS_INNER, 1, radians_of(col_outer * col_inner, COLUMN_LENGTH, 1))
    col_time = COLS_INNER * col_outer + col_inner
    values = dft_section(values, 'dimjy,iojx->domxy', COLS_OUTER, 1, radians_of(freq_row[:, None, None] * col_time[None], SEGMENT_SAMPLES, 1))
    values = values.reshape(trial_total, 2, ROWS_OUTER, ROWS_INNER, COLUMN_LENGTH)
    outer_pos = jnp.arange(ROWS_OUTER, dtype=jnp.int32)[:, None]
    inner_pos = jnp.arange(ROWS_INNER, dtype=jnp.int32)[None, :]
    values = dft_section(values, 'dikqb,ioqy->dokyb', ROWS_INNER, 1, radians_of(outer_pos * inner_pos, ROW_LENGTH, 1)[:, :, None])
    values = dft_section(values, 'dikyb,iokx->doxyb', ROWS_OUTER, 1, None)
    wide = values.reshape(trial_total, 2, ROW_LENGTH, COLUMN_LENGTH).astype(jnp.float32)
    detected_power = wide[:, 0] * wide[:, 0] + wide[:, 1] * wide[:, 1]
    decimated_power = lax.optimization_barrier(jnp.mean(detected_power.reshape(trial_total, ROW_LENGTH, COLUMN_LENGTH // DECIMATE_FACTOR, DECIMATE_FACTOR), axis=3))
    return decimated_power.reshape(trial_total, SEGMENT_SAMPLES // DECIMATE_FACTOR)

def reference(baseband, spectrum_in, dm_index):
    spectrum_out = forward_spectrum(baseband)
    grid_steps = dm_index.astype(jnp.int32) + 1
    series_list = []
    for trial_pos in range(TRIALS):
        series_list.append(dedisperse(spectrum_in, grid_steps[trial_pos:trial_pos + 1]))
    series = jnp.concatenate(series_list, axis=0)
    padded = jnp.pad(series, ((0, 0), (HALF_WIDTH, HALF_WIDTH)))
    length = series.shape[1]
    window_sum = padded[:, 0:length]
    for offset in range(1, 2 * HALF_WIDTH + 1):
        window_sum = window_sum + padded[:, offset:offset + length]
    smoothed = window_sum / (2 * HALF_WIDTH + 1)
    return (spectrum_out, smoothed)
```

```python
import functools
import math

import jax
import jax.numpy as jnp
import numpy as np
from jax import lax
from jax.experimental import pallas as pl
from jax.experimental.pallas import tpu as pltpu
from jax.sharding import PartitionSpec as P

ROWS_OUTER = 32
ROWS_INNER = 128
COLS_OUTER = 64
COLS_INNER = 128
ROW_LENGTH = 4096
COLUMN_LENGTH = 8192
SEGMENT_SAMPLES = 33554432
DM_GRID = 64
DECIMATE_FACTOR = 16
HALF_WIDTH = 16
LANES = 128
MESH = pl.DeviceIdType.MESH
F32 = jnp.float32
BF16 = jnp.bfloat16


def table(length, direction):
    product = np.outer(np.arange(length), np.arange(length)) % length
    radians = np.float32(direction * 2.0 * math.pi / length) * product.astype(np.float32)
    scale = np.float32(1.0 / math.sqrt(length))
    cosine = np.cos(radians).astype(np.float32) * scale
    sine = np.sin(radians).astype(np.float32) * scale
    return np.stack([np.stack([cosine, sine]), np.stack([-sine, cosine])])


def left_matrix(length, direction, parts_inner=False):
    t = table(length, direction).transpose(1, 3, 0, 2)
    if parts_inner:
        t = t.transpose(0, 1, 3, 2)
    return jnp.asarray(t.reshape(2 * length, 2 * length), BF16)


def right_matrix(length, direction):
    return jnp.asarray(table(length, direction).transpose(0, 2, 1, 3).reshape(2 * length, 2 * length), BF16)


def cos_sin(turns):
    quarter = jnp.round(turns * 4.0)
    theta = (turns - quarter * 0.25) * (2.0 * math.pi)
    z = theta * theta
    s = theta * (1.0 + z * (-1.0 / 6 + z * (1.0 / 120 + z * (-1.0 / 5040 + z * (1.0 / 362880)))))
    c = 1.0 + z * (-0.5 + z * (1.0 / 24 + z * (-1.0 / 720 + z * (1.0 / 40320))))
    q = quarter.astype(jnp.int32)
    odd = (q & 1) == 1
    cc = jnp.where(odd, s, c)
    ss = jnp.where(odd, c, s)
    cc = jnp.where(((q + 1) & 2) == 2, -cc, cc)
    ss = jnp.where((q & 2) == 2, -ss, ss)
    return cc, ss


def unit(numer, modulus):
    half = modulus // 2
    centred = ((numer + half) & (modulus - 1)) - half
    return cos_sin(centred.astype(F32) * (1.0 / modulus))


def iota(shape, dim):
    return lax.broadcasted_iota(jnp.int32, shape, dim)


def dot(a, b):
    return jnp.dot(a, b, preferred_element_type=F32)


def order(i, chips):
    t = chips - 1 - i
    odd = lax.rem(t, 2)
    return odd * lax.div(t + 1, 2) + (1 - odd) * (chips - lax.div(t, 2))


def kernel(
    n, rows, axis,
    dm_ref, xb, spec, m1f, m2f, m3f, m4f, m1i, m2i, m3i, m4i,
    out_ref, smooth_ref,
    spec_v, r1, r2, r3, s2, s3, fa, fb, sd, ra, rb, tb, halo, tpad, sm, twc, tws,
    send1, recv1, send2, recv2, send3, recv3, send_d, recv_d, misc,
):
    me = lax.axis_index(axis)
    chips = n // 2
    z = lax.div(me, 2)
    core = lax.rem(me, 2)

    def peer(i):
        dz = order(lax.div(i, 2), chips)
        dc = 1 - lax.rem(i, 2)
        return lax.rem(z + dz, chips) * 2 + lax.rem(core + dc, 2)

    load_spec = pltpu.make_async_copy(spec, spec_v, misc.at[0])
    load_spec.start()
    load_own = pltpu.make_async_copy(xb.at[me], r1.at[me], misc.at[1])
    load_own.start()

    barrier = pltpu.get_barrier_semaphore()

    @pl.loop(0, n - 1)
    def _(i):
        pl.semaphore_signal(barrier, inc=1, device_id={axis: peer(i)}, device_id_type=MESH)

    pl.semaphore_wait(barrier, n - 1)

    def remote(src, dst, send, recv, target):
        return pltpu.make_async_remote_copy(
            src_ref=src, dst_ref=dst, send_sem=send, recv_sem=recv,
            device_id={axis: target}, device_id_type=MESH,
        )

    def first(i):
        x = peer(i)
        return remote(xb.at[x], r1.at[me], send1.at[i], recv1.at[i], x)

    @pl.loop(0, n - 1)
    def _(i):
        first(i).start()

    m_iota = iota((rows, LANES), 0)
    lane = iota((rows, LANES), 1)
    freq_row = z + ROWS_OUTER * (rows * core + m_iota)
    steps = dm_ref[0] + 1
    row_turns = (steps * freq_row * freq_row).astype(F32) * (2.0 ** -33)
    load_spec.wait()

    @pl.loop(0, COLS_OUTER)
    def _(c):
        at = pl.ds(pl.multiple_of(c * LANES, LANES), LANES)
        re = spec_v[0, :, at].astype(F32)
        im = spec_v[1, :, at].astype(F32)
        col = c + COLS_OUTER * lane
        cross = (steps * (freq_row * col)) & (2 * DM_GRID * COLUMN_LENGTH - 1)
        square = (steps * ((col * col) & 511)) & 511
        turns = row_turns + cross.astype(F32) * (0.5 / (DM_GRID * COLUMN_LENGTH)) + square.astype(F32) * (1.0 / 512)
        co, si = cos_sin(turns)
        a = jnp.concatenate([(re * co - im * si).astype(BF16), (re * si + im * co).astype(BF16)], axis=1)
        w = dot(a, m4i[...])
        wr, wi = w[:, :LANES], w[:, LANES:]
        co, si = unit(c * lane, COLUMN_LENGTH)
        fa[pl.ds(pl.multiple_of(c * rows, rows), rows), :] = wr * co - wi * si
        fa[pl.ds(pl.multiple_of((COLS_OUTER + c) * rows, rows), rows), :] = wr * si + wi * co

    half = iota((COLS_OUTER, LANES), 0)
    half_lane = iota((COLS_OUTER, LANES), 1)

    @pl.loop(0, rows)
    def _(m):
        x = fa[pl.ds(m, 2 * COLS_OUTER, stride=rows), :].astype(BF16)
        w = dot(m3i[...], x)
        wr, wi = w[:COLS_OUTER], w[COLS_OUTER:]
        k = z + ROWS_OUTER * (rows * core + m)
        co, si = unit((LANES * half + half_lane) * k, SEGMENT_SAMPLES)
        fb[pl.ds(m, COLS_OUTER, stride=2 * rows), :] = wr * co - wi * si
        fb[pl.ds(rows + m, COLS_OUTER, stride=2 * rows), :] = wr * si + wi * co

    def second(i):
        x = peer(i)
        return remote(s2.at[x], r2.at[me], send2.at[i], recv2.at[i], x)

    @pl.loop(0, n - 1)
    def _(i):
        x = peer(i)
        s2[x] = fb[pl.ds(pl.multiple_of(x * 2 * rows, 2 * rows), 2 * rows), :].astype(BF16)
        second(i).start()

    r2[me] = fb[pl.ds(pl.multiple_of(me * 2 * rows, 2 * rows), 2 * rows), :].astype(BF16)

    load_own.wait()

    @pl.loop(0, n - 1)
    def _(i):
        first(i).wait_recv()

    @pl.loop(0, n)
    def _(d):
        fa[pl.ds(pl.multiple_of(d * 2 * rows, 2 * rows), 2 * rows), :] = r1[d].astype(F32)

    p_iota = iota((ROWS_OUTER, LANES), 0)

    @pl.loop(0, rows)
    def _(j):
        def columns(g):
            start = g * 2 * rows + j
            parts = [fa[pl.ds(start + part * rows, ROWS_OUTER, stride=4 * rows), :] for part in range(2)]
            return jnp.concatenate(parts, axis=0).astype(BF16)

        u = dot(m1f[...], jnp.concatenate([columns(0), columns(1)], axis=1))
        for g in range(2):
            n2 = g * rows + j
            ur = u[:ROWS_OUTER, g * LANES : (g + 1) * LANES]
            ui = u[ROWS_OUTER:, g * LANES : (g + 1) * LANES]
            co, si = unit(p_iota * n2, ROW_LENGTH)
            fb[pl.ds(n2, ROWS_OUTER, stride=ROWS_INNER), :] = ur * co + ui * si
            fb[pl.ds(ROW_LENGTH + n2, ROWS_OUTER, stride=ROWS_INNER), :] = ui * co - ur * si

    q_iota = iota((ROWS_INNER, LANES), 0)
    q_lane = iota((ROWS_INNER, LANES), 1)

    def third(i):
        x = peer(i)
        return remote(s3.at[x], r3.at[me], send3.at[i], recv3.at[i], x)

    @pl.loop(0, chips)
    def _(i):
        p = lax.rem(z + order(i, chips), chips)
        at = pl.multiple_of(p * ROWS_INNER, ROWS_INNER)
        x = jnp.concatenate(
            [fb[pl.ds(at, ROWS_INNER), :].astype(BF16), fb[pl.ds(ROW_LENGTH + at, ROWS_INNER), :].astype(BF16)], axis=0
        )
        u = dot(m2f[...], x)
        ur, ui = u[:ROWS_INNER], u[ROWS_INNER:]
        co, si = unit((LANES * me + q_lane) * (p + ROWS_OUTER * q_iota), SEGMENT_SAMPLES)
        re = (ur * co + ui * si).astype(BF16)
        im = (ui * co - ur * si).astype(BF16)
        for h in range(2):
            s3[2 * p + h, :rows, :] = re[h * rows : (h + 1) * rows]
            s3[2 * p + h, rows:, :] = im[h * rows : (h + 1) * rows]
        third(2 * i).start()

        @pl.when(i < chips - 1)
        def _():
            third(2 * i + 1).start()

    r3[me] = s3[me]

    @pl.loop(0, n - 1)
    def _(i):
        second(i).wait_recv()

    @pl.loop(0, chips)
    def _(p):
        x = jnp.concatenate(
            [r2[2 * p, :rows, :], r2[2 * p + 1, :rows, :], r2[2 * p, rows:, :], r2[2 * p + 1, rows:, :]], axis=0
        )
        w = dot(m2i[...], x)
        wr, wi = w[:ROWS_INNER], w[ROWS_INNER:]
        co, si = unit(p * q_iota, ROW_LENGTH)
        at = pl.multiple_of(p * ROWS_INNER, ROWS_INNER)
        fa[pl.ds(at, ROWS_INNER), :] = wr * co - wi * si
        fa[pl.ds(ROW_LENGTH + at, ROWS_INNER), :] = wr * si + wi * co

    @pl.loop(0, rows)
    def _(j):
        x = jnp.concatenate(
            [fa[pl.ds(g * rows + j, 2 * ROWS_OUTER, stride=ROWS_INNER), :].astype(BF16) for g in range(2)], axis=1
        )
        w = dot(m1i[...], x).astype(BF16).astype(F32)
        power = w[:ROWS_OUTER] * w[:ROWS_OUTER] + w[ROWS_OUTER:] * w[ROWS_OUTER:]
        for g in range(2):
            fb[pl.ds(g * rows + j, ROWS_OUTER, stride=ROWS_INNER), :] = power[:, g * LANES : (g + 1) * LANES]

    groups = LANES // DECIMATE_FACTOR
    mean = (iota((groups, LANES), 1) // DECIMATE_FACTOR == iota((groups, LANES), 0)).astype(F32).astype(BF16)

    def averaged(at):
        power = fb[pl.ds(pl.multiple_of(at * ROWS_INNER, ROWS_INNER), ROWS_INNER), :]
        high = power.astype(BF16)
        low = (power - high.astype(F32)).astype(BF16)
        total = sum(
            lax.dot_general(mean, part, (((1,), (1,)), ((), ())), preferred_element_type=F32) for part in (high, low)
        )
        return (total * (1.0 / DECIMATE_FACTOR)).astype(BF16)

    def detected(i):
        x = lax.rem(z + order(i, chips), chips)
        return remote(sd.at[x], ra.at[z], send_d.at[i], recv_d.at[i], 2 * x + core)

    @pl.loop(0, chips - 1)
    def _(i):
        x = lax.rem(z + order(i, chips), chips)
        sd[x] = averaged(x)
        detected(i).start()

    ra[z] = averaged(z)

    @pl.loop(0, chips - 1)
    def _(i):
        detected(i).wait_recv()

    swap = remote(ra, rb, misc.at[2], misc.at[3], 2 * z + 1 - core)
    swap.start()
    swap.wait_recv()

    @pl.loop(0, chips)
    def _(i):
        own = pl.multiple_of(groups * (2 * i + core), groups)
        other = pl.multiple_of(groups * (2 * i + 1 - core), groups)
        tpad[pl.ds(HALF_WIDTH + own, groups), :] = ra[i].astype(F32)
        tpad[pl.ds(HALF_WIDTH + other, groups), :] = rb[i].astype(F32)

    series = groups * n
    tb[0] = tpad[HALF_WIDTH : 2 * HALF_WIDTH, :].astype(BF16)
    tb[1] = tpad[series : series + HALF_WIDTH, :].astype(BF16)
    aside = lax.rem(z + core + (1 - core) * (chips - 1), chips)
    edge = remote(tb.at[core], halo, misc.at[4], misc.at[5], 2 * aside + 1 - core)
    edge.start()
    edge.wait_recv()
    inside = ((z > 0) | (core == 1)) & ((z < chips - 1) | (core == 0))
    got = jnp.where(inside, halo[...].astype(F32), 0.0)
    edge_lane = iota((HALF_WIDTH, LANES), 1)
    above = jnp.where(edge_lane == 0, pltpu.roll(got, 1, 1), pltpu.roll(tpad[series : series + HALF_WIDTH, :], 1, 1))
    below = jnp.where(
        edge_lane == LANES - 1,
        pltpu.roll(got, LANES - 1, 1),
        pltpu.roll(tpad[HALF_WIDTH : 2 * HALF_WIDTH, :], LANES - 1, 1),
    )
    tpad[:HALF_WIDTH, :] = above
    tpad[series + HALF_WIDTH :, :] = below
    width = 2 * HALF_WIDTH

    @pl.loop(0, series // LANES)
    def _(i):
        at = pl.multiple_of(i * LANES, LANES)
        offset = iota((LANES, LANES + width), 1) - iota((LANES, LANES + width), 0)
        band = jnp.where((offset >= 0) & (offset <= width), 1.0, 0.0).astype(BF16)
        total = dot(band, tpad[pl.ds(at, LANES + width), :].astype(BF16))
        sm[:, pl.ds(at, LANES)] = total.T / (width + 1.0)

    smooth_ref[...] = sm[pl.ds(pl.multiple_of(core * rows, rows), rows), :]

    co, si = unit(half * half_lane, COLUMN_LENGTH)
    twc[...] = co
    tws[...] = si

    @pl.loop(0, n - 1)
    def _(i):
        third(i).wait_recv()

    @pl.loop(0, n)
    def _(d):
        fa[pl.ds(pl.multiple_of(d * 2 * rows, 2 * rows), 2 * rows), :] = r3[d].astype(F32)

    @pl.loop(0, rows)
    def _(m):
        x = fa[pl.ds(m, 2 * n, stride=rows), :].astype(BF16)
        v = dot(m3f[...], x)
        vr, vi = v[:COLS_OUTER], v[COLS_OUTER:]
        co, si = twc[...], tws[...]
        fb[pl.ds(m, COLS_OUTER, stride=rows), :] = vr * co + vi * si
        fb[pl.ds(COLS_OUTER * rows + m, COLS_OUTER, stride=rows), :] = vi * co - vr * si

    @pl.loop(0, COLS_OUTER)
    def _(c):
        at = pl.multiple_of(c * rows, rows)
        a = jnp.concatenate(
            [fb[pl.ds(at, rows), :].astype(BF16), fb[pl.ds(COLS_OUTER * rows + at, rows), :].astype(BF16)], axis=1
        )
        v = dot(a, m4f[...]).astype(BF16)
        lanes = pl.ds(pl.multiple_of(c * LANES, LANES), LANES)
        out_ref[0, :, lanes] = v[:, :LANES]
        out_ref[1, :, lanes] = v[:, LANES:]

    @pl.loop(0, n - 1)
    def _(i):
        first(i).wait_send()
        second(i).wait_send()
        third(i).wait_send()

    @pl.loop(0, chips - 1)
    def _(i):
        detected(i).wait_send()

    swap.wait_send()
    edge.wait_send()


def on_device(n, baseband, spectrum_in, dm_index):
    rows = spectrum_in.shape[1]
    chips = n // 2
    assert (rows * n, chips, n) == (ROW_LENGTH, ROWS_OUTER, COLS_OUTER)
    groups = LANES // DECIMATE_FACTOR
    blocks = baseband.reshape(2, rows, n, LANES).transpose(2, 0, 1, 3).reshape(n, 2 * rows, LANES)
    matrices = (
        left_matrix(ROWS_OUTER, -1), left_matrix(ROWS_INNER, -1),
        left_matrix(COLS_OUTER, -1, True), right_matrix(COLS_INNER, -1),
        left_matrix(ROWS_OUTER, 1), left_matrix(ROWS_INNER, 1),
        left_matrix(COLS_OUTER, 1), right_matrix(COLS_INNER, 1),
    )
    block = pltpu.VMEM((n, 2 * rows, LANES), BF16)
    floats = pltpu.VMEM((n * 2 * rows, LANES), F32)
    dma = pltpu.SemaphoreType.DMA
    anywhere = pl.BlockSpec(memory_space=pl.ANY)
    vmem = pl.BlockSpec(memory_space=pltpu.VMEM)
    spectrum_out, smoothed = pl.pallas_call(
        functools.partial(kernel, n, rows, "fft"),
        out_shape=(
            jax.ShapeDtypeStruct(spectrum_in.shape, BF16),
            jax.ShapeDtypeStruct((rows, groups * n), F32),
        ),
        in_specs=[pl.BlockSpec(memory_space=pltpu.SMEM), anywhere, anywhere] + [vmem] * 8,
        out_specs=(vmem, vmem),
        scratch_shapes=[
            pltpu.VMEM(spectrum_in.shape, BF16), block, block, block, block, block, floats, floats,
            pltpu.VMEM((chips, groups, LANES), BF16), pltpu.VMEM((chips, groups, LANES), BF16),
            pltpu.VMEM((chips, groups, LANES), BF16), pltpu.VMEM((2, HALF_WIDTH, LANES), BF16),
            pltpu.VMEM((HALF_WIDTH, LANES), BF16), pltpu.VMEM((groups * n + 2 * HALF_WIDTH, LANES), F32),
            pltpu.VMEM((LANES, groups * n), F32),
            pltpu.VMEM((COLS_OUTER, LANES), F32), pltpu.VMEM((COLS_OUTER, LANES), F32),
            dma((n,)), dma((n,)), dma((n,)), dma((n,)), dma((n,)), dma((n,)), dma((chips,)), dma((chips,)), dma((6,)),
        ],
        compiler_params=pltpu.CompilerParams(
            collective_id=0, has_side_effects=True, vmem_limit_bytes=60 * 2**20
        ),
        name="dedisperse",
    )(dm_index, blocks, spectrum_in, *matrices)
    return spectrum_out, smoothed.reshape(1, -1)


def solution(mesh):
    return jax.shard_map(
        functools.partial(on_device, mesh.shape["fft"]),
        mesh=mesh,
        in_specs=(P("beam", "fft"), P("beam", "fft", None), P()),
        out_specs=(P("beam", "fft", None), P("beam", "fft")),
        check_vma=False,
    )
```

```python
import functools
import math

import jax
import jax.numpy as jnp
import numpy as np
from jax import lax
from jax.experimental import pallas as pl
from jax.experimental.pallas import tpu as pltpu
from jax.sharding import PartitionSpec as P

ROWS_OUTER = 32
ROWS_INNER = 128
COLS_OUTER = 64
COLS_INNER = 128
ROW_LENGTH = 4096
COLUMN_LENGTH = 8192
SEGMENT_SAMPLES = 33554432
DM_GRID = 64
DECIMATE_FACTOR = 16
HALF_WIDTH = 16
LANES = 128
MESH = pl.DeviceIdType.MESH
BATCHES = ((0, 4), (4, 2), (6, 1), (7, 1))
F32 = jnp.float32
BF16 = jnp.bfloat16


def table(length, direction):
    product = np.outer(np.arange(length), np.arange(length)) % length
    radians = np.float32(direction * 2.0 * math.pi / length) * product.astype(np.float32)
    scale = np.float32(1.0 / math.sqrt(length))
    cosine = np.cos(radians).astype(np.float32) * scale
    sine = np.sin(radians).astype(np.float32) * scale
    return np.stack([np.stack([cosine, sine]), np.stack([-sine, cosine])])


def left_matrix(length, direction):
    return jnp.asarray(table(length, direction).transpose(1, 3, 0, 2).reshape(2 * length, 2 * length), BF16)


def right_matrix(length, direction):
    return jnp.asarray(table(length, direction).transpose(0, 2, 1, 3).reshape(2 * length, 2 * length), BF16)


def cos_sin(turns):
    quarter = jnp.round(turns * 4.0)
    theta = (turns - quarter * 0.25) * (2.0 * math.pi)
    z = theta * theta
    s = theta * (1.0 + z * (-1.0 / 6 + z * (1.0 / 120 + z * (-1.0 / 5040 + z * (1.0 / 362880)))))
    c = 1.0 + z * (-0.5 + z * (1.0 / 24 + z * (-1.0 / 720 + z * (1.0 / 40320))))
    q = quarter.astype(jnp.int32)
    odd = (q & 1) == 1
    cc = jnp.where(odd, s, c)
    ss = jnp.where(odd, c, s)
    cc = jnp.where(((q + 1) & 2) == 2, -cc, cc)
    ss = jnp.where((q & 2) == 2, -ss, ss)
    return cc, ss


def unit(numer, modulus):
    half = modulus // 2
    centred = ((numer + half) & (modulus - 1)) - half
    return cos_sin(centred.astype(F32) * (1.0 / modulus))


def iota(shape, dim):
    return lax.broadcasted_iota(jnp.int32, shape, dim)


def dot(a, b):
    return jnp.dot(a, b, preferred_element_type=F32)


def order(i, chips):
    t = chips - 1 - i
    odd = lax.rem(t, 2)
    return odd * lax.div(t + 1, 2) + (1 - odd) * (chips - lax.div(t, 2))


def kernel(
    n, rows, axis,
    dm_ref, xb, spec, h1f, h2f, h3f, h4f, h1i, h2i, h3i, h4i,
    out_ref, smooth_ref,
    m1f, m2f, m3f, m4f, m1i, m2i, m3i, m4i, spec_v, r1, r2, r3, s2, s3, fa, fb, sd, ra, rb, tb, halo, tpad, sm, twc, tws,
    send1, recv1, send2, recv2, send3, recv3, send_d, recv_d, misc, loaded, ready,
):
    me = lax.axis_index(axis)
    chips = n // 2
    z = lax.div(me, 2)
    core = lax.rem(me, 2)

    def peer(i):
        dz = order(lax.div(i, 2), chips)
        dc = 1 - lax.rem(i, 2)
        return lax.rem(z + dz, chips) * 2 + lax.rem(core + dc, 2)

    load_spec = pltpu.make_async_copy(spec, spec_v, misc.at[0])
    load_own = pltpu.make_async_copy(xb.at[:, me], r1.at[me], misc.at[1])
    pairs = zip((h1f, h2f, h3f, h4f, h1i, h2i, h3i, h4i), (m1f, m2f, m3f, m4f, m1i, m2i, m3i, m4i))
    loads = [load_spec] + [pltpu.make_async_copy(h, m, loaded.at[i]) for i, (h, m) in enumerate(pairs)]
    for load in loads:
        load.start()
    load_own.start()

    barrier = pltpu.get_barrier_semaphore()

    near, middle = 2 * (chips - 1 - chips // 4), 2 * (chips - 1 - chips // 2)

    @pl.loop(near, n - 1)
    def _(i):
        pl.semaphore_signal(barrier, inc=1, device_id={axis: peer(i)}, device_id_type=MESH)

    pl.semaphore_wait(barrier, n - 1 - near)

    def remote(src, dst, send, recv, target):
        return pltpu.make_async_remote_copy(
            src_ref=src, dst_ref=dst, send_sem=send, recv_sem=recv,
            device_id={axis: target}, device_id_type=MESH,
        )

    def first(i):
        x = peer(i)
        return remote(xb.at[:, x], r1.at[me], send1.at[i], recv1.at[i], x)

    def send_first(start, stop):
        @pl.loop(start, stop)
        def _(i):
            first(i).start()

    send_first(near, n - 1)
    for level, (reach, start, stop) in enumerate(((chips // 8, middle, near), (chips // 4, 0, middle))):
        for side in (reach, chips - reach):
            target = 2 * lax.rem(z + side, chips) + core
            pl.semaphore_signal(ready.at[level], inc=1, device_id={axis: target}, device_id_type=MESH)
        pl.semaphore_wait(ready.at[level], 2)
        send_first(start, stop)

    m_iota = iota((rows, LANES), 0)
    lane = iota((rows, LANES), 1)
    freq_row = z + ROWS_OUTER * (rows * core + m_iota)
    steps = dm_ref[0] + 1
    row_turns = (steps * freq_row * freq_row).astype(F32) * (2.0 ** -33)
    for load in loads:
        load.wait()

    @pl.loop(0, COLS_OUTER)
    def _(c):
        at = pl.ds(pl.multiple_of(c * LANES, LANES), LANES)
        re = spec_v[0, :, at].astype(F32)
        im = spec_v[1, :, at].astype(F32)
        col = c + COLS_OUTER * lane
        cross = (steps * (freq_row * col)) & (2 * DM_GRID * COLUMN_LENGTH - 1)
        square = (steps * ((col * col) & 511)) & 511
        turns = row_turns + cross.astype(F32) * (0.5 / (DM_GRID * COLUMN_LENGTH)) + square.astype(F32) * (1.0 / 512)
        co, si = cos_sin(turns)
        a = jnp.concatenate([(re * co - im * si).astype(BF16), (re * si + im * co).astype(BF16)], axis=1)
        w = dot(a, m4i[...])
        wr, wi = w[:, :LANES], w[:, LANES:]
        co, si = unit(c * lane, COLUMN_LENGTH)
        fa[pl.ds(pl.multiple_of(c * rows, rows), rows), :] = wr * co - wi * si
        fa[pl.ds(pl.multiple_of((COLS_OUTER + c) * rows, rows), rows), :] = wr * si + wi * co

    half = iota((COLS_OUTER, LANES), 0)
    half_lane = iota((COLS_OUTER, LANES), 1)

    @pl.loop(0, rows)
    def _(m):
        x = fa[pl.ds(m, 2 * COLS_OUTER, stride=rows), :].astype(BF16)
        w = dot(m3i[...], x)
        wr, wi = w[:COLS_OUTER], w[COLS_OUTER:]
        k = z + ROWS_OUTER * (rows * core + m)
        co, si = unit((LANES * half + half_lane) * k, SEGMENT_SAMPLES)
        fb[pl.ds(m, COLS_OUTER, stride=2 * rows), :] = wr * co - wi * si
        fb[pl.ds(rows + m, COLS_OUTER, stride=2 * rows), :] = wr * si + wi * co

    def second(i):
        x = peer(i)
        return remote(s2.at[x], r2.at[me], send2.at[i], recv2.at[i], x)

    @pl.loop(0, n - 1)
    def _(i):
        x = peer(i)
        s2[x] = fb[pl.ds(pl.multiple_of(x * 2 * rows, 2 * rows), 2 * rows), :].astype(BF16)
        second(i).start()

    r2[me] = fb[pl.ds(pl.multiple_of(me * 2 * rows, 2 * rows), 2 * rows), :].astype(BF16)

    load_own.wait()

    @pl.loop(0, n - 1)
    def _(i):
        first(i).wait_recv()

    @pl.loop(0, n)
    def _(d):
        fa[pl.ds(pl.multiple_of(d * 2 * rows, 2 * rows), 2 * rows), :] = r1[d].astype(F32).reshape(2 * rows, LANES)

    p_iota = iota((ROWS_OUTER, LANES), 0)

    @pl.loop(0, rows)
    def _(j):
        def columns(g):
            start = g * 2 * rows + 2 * j
            parts = [fa[pl.ds(start + part, ROWS_OUTER, stride=4 * rows), :] for part in range(2)]
            return jnp.concatenate(parts, axis=0).astype(BF16)

        u = dot(m1f[...], jnp.concatenate([columns(0), columns(1)], axis=1))
        for g in range(2):
            n2 = g * rows + j
            ur = u[:ROWS_OUTER, g * LANES : (g + 1) * LANES]
            ui = u[ROWS_OUTER:, g * LANES : (g + 1) * LANES]
            co, si = unit(p_iota * n2, ROW_LENGTH)
            fb[pl.ds(n2, ROWS_OUTER, stride=ROWS_INNER), :] = ur * co + ui * si
            fb[pl.ds(ROW_LENGTH + n2, ROWS_OUTER, stride=ROWS_INNER), :] = ui * co - ur * si

    q_iota = iota((ROWS_INNER, LANES), 0)
    q_lane = iota((ROWS_INNER, LANES), 1)

    def third(batch, i):
        x = peer(i)
        first_group, count = BATCHES[batch]
        at = pl.ds(16 * first_group, 16 * count)
        step = batch * n + i
        return remote(s3.at[x, at], r3.at[me, at], send3.at[step], recv3.at[step], x)

    @pl.loop(0, chips)
    def _(i):
        p = lax.rem(z + order(i, chips), chips)
        at = pl.multiple_of(p * ROWS_INNER, ROWS_INNER)
        x = jnp.concatenate(
            [fb[pl.ds(at, ROWS_INNER), :].astype(BF16), fb[pl.ds(ROW_LENGTH + at, ROWS_INNER), :].astype(BF16)], axis=0
        )
        u = dot(m2f[...], x)
        ur, ui = u[:ROWS_INNER], u[ROWS_INNER:]
        co, si = unit((LANES * me + q_lane) * (p + ROWS_OUTER * q_iota), SEGMENT_SAMPLES)
        re = (ur * co + ui * si).reshape(2 * rows // 8, 1, 8, LANES)
        im = (ui * co - ur * si).reshape(2 * rows // 8, 1, 8, LANES)
        both = jnp.concatenate([re, im], axis=1).reshape(4 * rows, LANES).astype(BF16)
        s3[2 * p] = both[: 2 * rows]
        s3[2 * p + 1] = both[2 * rows :]
        third(0, 2 * i).start()

        @pl.when(i < chips - 1)
        def _():
            third(0, 2 * i + 1).start()

    r3[me] = s3[me]

    @pl.loop(0, n - 1)
    def _(i):
        second(i).wait_recv()

    @pl.loop(0, chips)
    def _(p):
        x = jnp.concatenate(
            [r2[2 * p, :rows, :], r2[2 * p + 1, :rows, :], r2[2 * p, rows:, :], r2[2 * p + 1, rows:, :]], axis=0
        )
        w = dot(m2i[...], x)
        wr, wi = w[:ROWS_INNER], w[ROWS_INNER:]
        co, si = unit(p * q_iota, ROW_LENGTH)
        at = pl.multiple_of(p * ROWS_INNER, ROWS_INNER)
        fa[pl.ds(at, ROWS_INNER), :] = wr * co - wi * si
        fa[pl.ds(ROW_LENGTH + at, ROWS_INNER), :] = wr * si + wi * co

    @pl.loop(0, rows)
    def _(j):
        x = jnp.concatenate(
            [fa[pl.ds(g * rows + j, 2 * ROWS_OUTER, stride=ROWS_INNER), :].astype(BF16) for g in range(2)], axis=1
        )
        w = dot(m1i[...], x).astype(BF16).astype(F32)
        power = w[:ROWS_OUTER] * w[:ROWS_OUTER] + w[ROWS_OUTER:] * w[ROWS_OUTER:]
        for g in range(2):
            fb[pl.ds(g * rows + j, ROWS_OUTER, stride=ROWS_INNER), :] = power[:, g * LANES : (g + 1) * LANES]

    groups = LANES // DECIMATE_FACTOR
    mean = (iota((groups, LANES), 1) // DECIMATE_FACTOR == iota((groups, LANES), 0)).astype(F32).astype(BF16)

    def averaged(at):
        power = fb[pl.ds(pl.multiple_of(at * ROWS_INNER, ROWS_INNER), ROWS_INNER), :]
        high = power.astype(BF16)
        low = (power - high.astype(F32)).astype(BF16)
        total = sum(
            lax.dot_general(mean, part, (((1,), (1,)), ((), ())), preferred_element_type=F32) for part in (high, low)
        )
        return (total * (1.0 / DECIMATE_FACTOR)).astype(BF16)

    def detected(i):
        x = lax.rem(z + order(i, chips), chips)
        return remote(sd.at[x], ra.at[z], send_d.at[i], recv_d.at[i], 2 * x + core)

    @pl.loop(0, chips - 1)
    def _(i):
        x = lax.rem(z + order(i, chips), chips)
        sd[x] = averaged(x)
        detected(i).start()

    def send_batch(batch):
        @pl.loop(0, n - 1)
        def _(i):
            third(batch, i).start()

    send_batch(1)
    ra[z] = averaged(z)

    co, si = unit(half * half_lane, COLUMN_LENGTH)
    twc[...] = co
    tws[...] = si

    def columns_of(batch):
        @pl.loop(0, n - 1)
        def _(i):
            third(batch, i).wait_recv()

        first_group, count = BATCHES[batch]

        @pl.loop(first_group, first_group + count)
        def _(g):
            at = pl.ds(pl.multiple_of(16 * g, 16), 16)
            for d in range(n):
                fa[16 * d : 16 * (d + 1), :] = r3[d, at, :].astype(F32)
            co, si = twc[...], tws[...]
            for m in range(8):
                x = jnp.concatenate([fa[pl.ds(8 * part + m, n, stride=16), :] for part in range(2)], axis=0)
                v = dot(m3f[...], x.astype(BF16))
                vr, vi = v[:COLS_OUTER], v[COLS_OUTER:]
                fb[pl.ds(m, COLS_OUTER, stride=8), :] = vr * co + vi * si
                fb[pl.ds(8 * COLS_OUTER + m, COLS_OUTER, stride=8), :] = vi * co - vr * si
            a = jnp.concatenate(
                [fb[: 8 * COLS_OUTER, :].astype(BF16), fb[8 * COLS_OUTER : 16 * COLS_OUTER, :].astype(BF16)], axis=1
            )
            v = dot(a, m4f[...])
            at = pl.ds(pl.multiple_of(8 * g, 8), 8)
            for c in range(COLS_OUTER):
                for part in range(2):
                    block = v[8 * c : 8 * (c + 1), part * LANES : (part + 1) * LANES]
                    out_ref[part, at, c * LANES : (c + 1) * LANES] = block.astype(BF16)

    columns_of(0)

    @pl.loop(0, chips - 1)
    def _(i):
        detected(i).wait_recv()

    swap = remote(ra, rb, misc.at[2], misc.at[3], 2 * z + 1 - core)
    swap.start()
    swap.wait_recv()

    @pl.loop(0, chips)
    def _(i):
        own = pl.multiple_of(groups * (2 * i + core), groups)
        other = pl.multiple_of(groups * (2 * i + 1 - core), groups)
        tpad[pl.ds(HALF_WIDTH + own, groups), :] = ra[i].astype(F32)
        tpad[pl.ds(HALF_WIDTH + other, groups), :] = rb[i].astype(F32)

    series = groups * n
    tb[0] = tpad[HALF_WIDTH : 2 * HALF_WIDTH, :].astype(BF16)
    tb[1] = tpad[series : series + HALF_WIDTH, :].astype(BF16)
    aside = lax.rem(z + core + (1 - core) * (chips - 1), chips)
    edge = remote(tb.at[core], halo, misc.at[4], misc.at[5], 2 * aside + 1 - core)
    edge.start()
    for batch in range(2, len(BATCHES)):
        send_batch(batch)
    columns_of(1)
    edge.wait_recv()
    inside = ((z > 0) | (core == 1)) & ((z < chips - 1) | (core == 0))
    got = jnp.where(inside, halo[...].astype(F32), 0.0)
    edge_lane = iota((HALF_WIDTH, LANES), 1)
    above = jnp.where(edge_lane == 0, pltpu.roll(got, 1, 1), pltpu.roll(tpad[series : series + HALF_WIDTH, :], 1, 1))
    below = jnp.where(
        edge_lane == LANES - 1,
        pltpu.roll(got, LANES - 1, 1),
        pltpu.roll(tpad[HALF_WIDTH : 2 * HALF_WIDTH, :], LANES - 1, 1),
    )
    tpad[:HALF_WIDTH, :] = above
    tpad[series + HALF_WIDTH :, :] = below
    width = 2 * HALF_WIDTH

    @pl.loop(0, series // LANES)
    def _(i):
        at = pl.multiple_of(i * LANES, LANES)
        offset = iota((LANES, LANES + width), 1) - iota((LANES, LANES + width), 0)
        band = jnp.where((offset >= 0) & (offset <= width), 1.0, 0.0).astype(BF16)
        total = dot(band, tpad[pl.ds(at, LANES + width), :].astype(BF16))
        sm[:, pl.ds(at, LANES)] = total.T / (width + 1.0)

    own_rows = pl.ds(pl.multiple_of(core * rows, rows), rows)
    for i in range(series // LANES):
        smooth_ref[pl.ds(i, rows, stride=series // LANES), :] = sm[own_rows, i * LANES : (i + 1) * LANES]

    for batch in range(2, len(BATCHES)):
        columns_of(batch)

    @pl.loop(0, n - 1)
    def _(i):
        first(i).wait_send()
        second(i).wait_send()
        for batch in range(len(BATCHES)):
            third(batch, i).wait_send()

    @pl.loop(0, chips - 1)
    def _(i):
        detected(i).wait_send()

    swap.wait_send()
    edge.wait_send()


def on_device(n, baseband, spectrum_in, dm_index):
    rows = spectrum_in.shape[1]
    chips = n // 2
    assert (rows * n, chips, n) == (ROW_LENGTH, ROWS_OUTER, COLS_OUTER)
    groups = LANES // DECIMATE_FACTOR
    blocks = baseband.reshape(2, rows, n, LANES).transpose(1, 2, 0, 3)
    matrices = (
        left_matrix(ROWS_OUTER, -1), left_matrix(ROWS_INNER, -1),
        left_matrix(COLS_OUTER, -1), right_matrix(COLS_INNER, -1),
        left_matrix(ROWS_OUTER, 1), left_matrix(ROWS_INNER, 1),
        left_matrix(COLS_OUTER, 1), right_matrix(COLS_INNER, 1),
    )
    block = pltpu.VMEM((n, 2 * rows, LANES), BF16)
    floats = pltpu.VMEM((n * 2 * rows, LANES), F32)
    dma = pltpu.SemaphoreType.DMA
    hbm = pl.BlockSpec(memory_space=pltpu.HBM)
    vmem = pl.BlockSpec(memory_space=pltpu.VMEM)
    spectrum_out, smoothed = pl.pallas_call(
        functools.partial(kernel, n, rows, "fft"),
        out_shape=(
            jax.ShapeDtypeStruct(spectrum_in.shape, BF16),
            jax.ShapeDtypeStruct((rows * groups * n // LANES, LANES), F32),
        ),
        in_specs=[pl.BlockSpec(memory_space=pltpu.SMEM)] + [hbm] * 10,
        out_specs=(vmem, vmem),
        scratch_shapes=[pltpu.VMEM(m.shape, BF16) for m in matrices] + [
            pltpu.VMEM(spectrum_in.shape, BF16), pltpu.VMEM((n, rows, 2, LANES), BF16), block, block, block, block, floats, floats,
            pltpu.VMEM((chips, groups, LANES), BF16), pltpu.VMEM((chips, groups, LANES), BF16),
            pltpu.VMEM((chips, groups, LANES), BF16), pltpu.VMEM((2, HALF_WIDTH, LANES), BF16),
            pltpu.VMEM((HALF_WIDTH, LANES), BF16), pltpu.VMEM((groups * n + 2 * HALF_WIDTH, LANES), F32),
            pltpu.VMEM((LANES, groups * n), F32),
            pltpu.VMEM((COLS_OUTER, LANES), F32), pltpu.VMEM((COLS_OUTER, LANES), F32),
            dma((n,)), dma((n,)), dma((n,)), dma((n,)), dma((len(BATCHES) * n,)), dma((len(BATCHES) * n,)), dma((chips,)), dma((chips,)), dma((6,)), dma((8,)),
            pltpu.SemaphoreType.REGULAR((2,)),
        ],
        compiler_params=pltpu.CompilerParams(
            collective_id=0, has_side_effects=True, vmem_limit_bytes=36 * 2**20
        ),
        name="dedisperse",
    )(dm_index, *(pltpu.with_memory_space_constraint(a, pltpu.HBM) for a in (blocks, spectrum_in, *matrices)))
    return spectrum_out, smoothed.reshape(1, -1)


def solution(mesh):
    return jax.shard_map(
        functools.partial(on_device, mesh.shape["fft"]),
        mesh=mesh,
        in_specs=(P("beam", "fft"), P("beam", "fft", None), P()),
        out_specs=(P("beam", "fft", None), P("beam", "fft")),
        check_vma=False,
    )
```

```python
import functools
import math

import jax
import jax.numpy as jnp
import numpy as np
from jax import lax
from jax.experimental import pallas as pl
from jax.experimental.pallas import tpu as pltpu
from jax.sharding import PartitionSpec as P

ROWS_OUTER = 32
ROWS_INNER = 128
COLS_OUTER = 64
COLS_INNER = 128
ROW_LENGTH = 4096
COLUMN_LENGTH = 8192
SEGMENT_SAMPLES = 33554432
DM_GRID = 64
DECIMATE_FACTOR = 16
HALF_WIDTH = 16
LANES = 128
MESH = pl.DeviceIdType.MESH
BATCHES = ((0, 4), (4, 2), (6, 1), (7, 1))
F32 = jnp.float32
BF16 = jnp.bfloat16


def table(length, direction):
    product = np.outer(np.arange(length), np.arange(length)) % length
    radians = np.float32(direction * 2.0 * math.pi / length) * product.astype(np.float32)
    scale = np.float32(1.0 / math.sqrt(length))
    cosine = np.cos(radians).astype(np.float32) * scale
    sine = np.sin(radians).astype(np.float32) * scale
    return np.stack([np.stack([cosine, sine]), np.stack([-sine, cosine])])


def left_matrix(length, direction):
    return jnp.asarray(table(length, direction).transpose(1, 3, 0, 2).reshape(2 * length, 2 * length), BF16)


def right_matrix(length, direction):
    return jnp.asarray(table(length, direction).transpose(0, 2, 1, 3).reshape(2 * length, 2 * length), BF16)


def cos_sin(turns):
    quarter = jnp.round(turns * 4.0)
    theta = (turns - quarter * 0.25) * (2.0 * math.pi)
    z = theta * theta
    s = theta * (1.0 + z * (-1.0 / 6 + z * (1.0 / 120 + z * (-1.0 / 5040 + z * (1.0 / 362880)))))
    c = 1.0 + z * (-0.5 + z * (1.0 / 24 + z * (-1.0 / 720 + z * (1.0 / 40320))))
    q = quarter.astype(jnp.int32)
    odd = (q & 1) == 1
    cc = jnp.where(odd, s, c)
    ss = jnp.where(odd, c, s)
    cc = jnp.where(((q + 1) & 2) == 2, -cc, cc)
    ss = jnp.where((q & 2) == 2, -ss, ss)
    return cc, ss


def unit(numer, modulus):
    half = modulus // 2
    centred = ((numer + half) & (modulus - 1)) - half
    return cos_sin(centred.astype(F32) * (1.0 / modulus))


def iota(shape, dim):
    return lax.broadcasted_iota(jnp.int32, shape, dim)


def dot(a, b):
    return jnp.dot(a, b, preferred_element_type=F32)


def order(i, chips):
    t = chips - 1 - i
    odd = lax.rem(t, 2)
    return odd * lax.div(t + 1, 2) + (1 - odd) * (chips - lax.div(t, 2))


def kernel(
    n, rows, axis,
    dm_ref, xb, spec, h1f, h2f, h3f, h4f, h1i, h2i, h3i, h4i,
    out_ref, smooth_ref,
    m1f, m2f, m3f, m4f, m1i, m2i, m3i, m4i, spec_v, r1, r2, r3, s2, s3, fa, fb, sd, ra, rb, tb, halo, tpad, sm, twc, tws,
    sent, got, misc, loaded, ready,
):
    me = lax.axis_index(axis)
    chips = n // 2
    z = lax.div(me, 2)
    core = lax.rem(me, 2)

    def peer(i):
        dz = order(lax.div(i, 2), chips)
        dc = 1 - lax.rem(i, 2)
        return lax.rem(z + dz, chips) * 2 + lax.rem(core + dc, 2)

    load_spec = pltpu.make_async_copy(spec, spec_v, misc.at[0])
    load_own = pltpu.make_async_copy(xb.at[:, me], r1.at[me], misc.at[1])
    pairs = zip((h1f, h2f, h3f, h4f, h1i, h2i, h3i, h4i), (m1f, m2f, m3f, m4f, m1i, m2i, m3i, m4i))
    loads = [load_spec] + [pltpu.make_async_copy(h, m, loaded.at[i]) for i, (h, m) in enumerate(pairs)]
    for load in loads:
        load.start()
    load_own.start()

    barrier = pltpu.get_barrier_semaphore()

    def within(reach):
        return 2 * max(chips - 1 - 2 * reach, 0)

    near = within(1)

    @pl.loop(near, n - 1)
    def _(i):
        pl.semaphore_signal(barrier, inc=1, device_id={axis: peer(i)}, device_id_type=MESH)

    pl.semaphore_wait(barrier, n - 1 - near)

    def remote(src, dst, send, recv, target):
        return pltpu.make_async_remote_copy(
            src_ref=src, dst_ref=dst, send_sem=send, recv_sem=recv,
            device_id={axis: target}, device_id_type=MESH,
        )

    def whole(ref, number):
        return remote(ref, ref, sent.at[number], got.at[number], 2 * z + 1 - core)

    others = pl.ds(0, n - 1)

    def rows_of(batch):
        first_group, count = BATCHES[batch]
        return r3.at[others, pl.ds(16 * first_group, 16 * count)]

    def first(i):
        x = peer(i)
        return remote(xb.at[:, x], r1.at[me], sent.at[0], got.at[0], x)

    def send_first(start, stop):
        @pl.loop(start, stop)
        def _(i):
            first(i).start()

    send_first(near, n - 1)
    for level in range(int(math.log2(chips)) - 1):
        reach = 2**level
        for side in (reach, chips - reach):
            target = 2 * lax.rem(z + side, chips) + core
            pl.semaphore_signal(ready.at[level], inc=1, device_id={axis: target}, device_id_type=MESH)
        pl.semaphore_wait(ready.at[level], 2)
        send_first(within(2 * reach), within(reach))

    m_iota = iota((rows, LANES), 0)
    lane = iota((rows, LANES), 1)
    freq_row = z + ROWS_OUTER * (rows * core + m_iota)
    steps = dm_ref[0] + 1
    row_turns = (steps * freq_row * freq_row).astype(F32) * (2.0 ** -33)
    for load in loads:
        load.wait()

    @pl.loop(0, COLS_OUTER)
    def _(c):
        at = pl.ds(pl.multiple_of(c * LANES, LANES), LANES)
        re = spec_v[0, :, at].astype(F32)
        im = spec_v[1, :, at].astype(F32)
        col = c + COLS_OUTER * lane
        cross = (steps * (freq_row * col)) & (2 * DM_GRID * COLUMN_LENGTH - 1)
        square = (steps * ((col * col) & 511)) & 511
        turns = row_turns + cross.astype(F32) * (0.5 / (DM_GRID * COLUMN_LENGTH)) + square.astype(F32) * (1.0 / 512)
        co, si = cos_sin(turns)
        a = jnp.concatenate([(re * co - im * si).astype(BF16), (re * si + im * co).astype(BF16)], axis=1)
        w = dot(a, m4i[...])
        wr, wi = w[:, :LANES], w[:, LANES:]
        co, si = unit(c * lane, COLUMN_LENGTH)
        fa[pl.ds(pl.multiple_of(c * rows, rows), rows), :] = wr * co - wi * si
        fa[pl.ds(pl.multiple_of((COLS_OUTER + c) * rows, rows), rows), :] = wr * si + wi * co

    half = iota((COLS_OUTER, LANES), 0)
    half_lane = iota((COLS_OUTER, LANES), 1)

    @pl.loop(0, rows)
    def _(m):
        x = fa[pl.ds(m, 2 * COLS_OUTER, stride=rows), :].astype(BF16)
        w = dot(m3i[...], x)
        wr, wi = w[:COLS_OUTER], w[COLS_OUTER:]
        k = z + ROWS_OUTER * (rows * core + m)
        co, si = unit((LANES * half + half_lane) * k, SEGMENT_SAMPLES)
        fb[pl.ds(m, COLS_OUTER, stride=2 * rows), :] = wr * co - wi * si
        fb[pl.ds(rows + m, COLS_OUTER, stride=2 * rows), :] = wr * si + wi * co

    def second(i):
        x = peer(i)
        return remote(s2.at[x], r2.at[me], sent.at[1], got.at[1], x)

    @pl.loop(0, n - 1)
    def _(i):
        x = peer(i)
        s2[x] = fb[pl.ds(pl.multiple_of(x * 2 * rows, 2 * rows), 2 * rows), :].astype(BF16)
        second(i).start()

    r2[me] = fb[pl.ds(pl.multiple_of(me * 2 * rows, 2 * rows), 2 * rows), :].astype(BF16)

    load_own.wait()

    whole(r1.at[others], 0).wait_recv()

    @pl.loop(0, n)
    def _(d):
        fa[pl.ds(pl.multiple_of(d * 2 * rows, 2 * rows), 2 * rows), :] = r1[d].astype(F32).reshape(2 * rows, LANES)

    p_iota = iota((ROWS_OUTER, LANES), 0)

    @pl.loop(0, rows)
    def _(j):
        def columns(g):
            start = g * 2 * rows + 2 * j
            parts = [fa[pl.ds(start + part, ROWS_OUTER, stride=4 * rows), :] for part in range(2)]
            return jnp.concatenate(parts, axis=0).astype(BF16)

        u = dot(m1f[...], jnp.concatenate([columns(0), columns(1)], axis=1))
        for g in range(2):
            n2 = g * rows + j
            ur = u[:ROWS_OUTER, g * LANES : (g + 1) * LANES]
            ui = u[ROWS_OUTER:, g * LANES : (g + 1) * LANES]
            co, si = unit(p_iota * n2, ROW_LENGTH)
            fb[pl.ds(n2, ROWS_OUTER, stride=ROWS_INNER), :] = ur * co + ui * si
            fb[pl.ds(ROW_LENGTH + n2, ROWS_OUTER, stride=ROWS_INNER), :] = ui * co - ur * si

    q_iota = iota((ROWS_INNER, LANES), 0)
    q_lane = iota((ROWS_INNER, LANES), 1)

    def third(batch, i):
        x = peer(i)
        first_group, count = BATCHES[batch]
        at = pl.ds(16 * first_group, 16 * count)
        return remote(s3.at[x, at], r3.at[me, at], sent.at[3 + batch], got.at[3 + batch], x)

    @pl.loop(0, chips)
    def _(i):
        p = lax.rem(z + order(i, chips), chips)
        at = pl.multiple_of(p * ROWS_INNER, ROWS_INNER)
        x = jnp.concatenate(
            [fb[pl.ds(at, ROWS_INNER), :].astype(BF16), fb[pl.ds(ROW_LENGTH + at, ROWS_INNER), :].astype(BF16)], axis=0
        )
        u = dot(m2f[...], x)
        ur, ui = u[:ROWS_INNER], u[ROWS_INNER:]
        co, si = unit((LANES * me + q_lane) * (p + ROWS_OUTER * q_iota), SEGMENT_SAMPLES)
        re = (ur * co + ui * si).reshape(2 * rows // 8, 1, 8, LANES)
        im = (ui * co - ur * si).reshape(2 * rows // 8, 1, 8, LANES)
        both = jnp.concatenate([re, im], axis=1).reshape(4 * rows, LANES).astype(BF16)
        s3[2 * p] = both[: 2 * rows]
        s3[2 * p + 1] = both[2 * rows :]
        third(0, 2 * i).start()

        @pl.when(i < chips - 1)
        def _():
            third(0, 2 * i + 1).start()

    r3[me] = s3[me]

    whole(r2.at[others], 1).wait_recv()

    @pl.loop(0, chips)
    def _(p):
        x = jnp.concatenate(
            [r2[2 * p, :rows, :], r2[2 * p + 1, :rows, :], r2[2 * p, rows:, :], r2[2 * p + 1, rows:, :]], axis=0
        )
        w = dot(m2i[...], x)
        wr, wi = w[:ROWS_INNER], w[ROWS_INNER:]
        co, si = unit(p * q_iota, ROW_LENGTH)
        at = pl.multiple_of(p * ROWS_INNER, ROWS_INNER)
        fa[pl.ds(at, ROWS_INNER), :] = wr * co - wi * si
        fa[pl.ds(ROW_LENGTH + at, ROWS_INNER), :] = wr * si + wi * co

    @pl.loop(0, rows)
    def _(j):
        x = jnp.concatenate(
            [fa[pl.ds(g * rows + j, 2 * ROWS_OUTER, stride=ROWS_INNER), :].astype(BF16) for g in range(2)], axis=1
        )
        w = dot(m1i[...], x).astype(BF16).astype(F32)
        power = w[:ROWS_OUTER] * w[:ROWS_OUTER] + w[ROWS_OUTER:] * w[ROWS_OUTER:]
        for g in range(2):
            fb[pl.ds(g * rows + j, ROWS_OUTER, stride=ROWS_INNER), :] = power[:, g * LANES : (g + 1) * LANES]

    groups = LANES // DECIMATE_FACTOR
    mean = (iota((groups, LANES), 1) // DECIMATE_FACTOR == iota((groups, LANES), 0)).astype(F32).astype(BF16)

    def averaged(at):
        power = fb[pl.ds(pl.multiple_of(at * ROWS_INNER, ROWS_INNER), ROWS_INNER), :]
        high = power.astype(BF16)
        low = (power - high.astype(F32)).astype(BF16)
        total = sum(
            lax.dot_general(mean, part, (((1,), (1,)), ((), ())), preferred_element_type=F32) for part in (high, low)
        )
        return (total * (1.0 / DECIMATE_FACTOR)).astype(BF16)

    def detected(i):
        x = lax.rem(z + order(i, chips), chips)
        return remote(sd.at[x], ra.at[z], sent.at[2], got.at[2], 2 * x + core)

    @pl.loop(0, chips - 1)
    def _(i):
        x = lax.rem(z + order(i, chips), chips)
        sd[x] = averaged(x)
        detected(i).start()

    def send_batch(batch):
        @pl.loop(0, n - 1)
        def _(i):
            third(batch, i).start()

    send_batch(1)
    ra[z] = averaged(z)

    co, si = unit(half * half_lane, COLUMN_LENGTH)
    twc[...] = co
    tws[...] = si

    def columns_of(batch):
        whole(rows_of(batch), 3 + batch).wait_recv()
        first_group, count = BATCHES[batch]

        @pl.loop(first_group, first_group + count)
        def _(g):
            at = pl.ds(pl.multiple_of(16 * g, 16), 16)
            for d in range(n):
                fa[16 * d : 16 * (d + 1), :] = r3[d, at, :].astype(F32)
            co, si = twc[...], tws[...]
            for m in range(8):
                x = jnp.concatenate([fa[pl.ds(8 * part + m, n, stride=16), :] for part in range(2)], axis=0)
                v = dot(m3f[...], x.astype(BF16))
                vr, vi = v[:COLS_OUTER], v[COLS_OUTER:]
                fb[pl.ds(m, COLS_OUTER, stride=8), :] = vr * co + vi * si
                fb[pl.ds(8 * COLS_OUTER + m, COLS_OUTER, stride=8), :] = vi * co - vr * si
            a = jnp.concatenate(
                [fb[: 8 * COLS_OUTER, :].astype(BF16), fb[8 * COLS_OUTER : 16 * COLS_OUTER, :].astype(BF16)], axis=1
            )
            v = dot(a, m4f[...])
            at = pl.ds(pl.multiple_of(8 * g, 8), 8)
            for c in range(COLS_OUTER):
                for part in range(2):
                    block = v[8 * c : 8 * (c + 1), part * LANES : (part + 1) * LANES]
                    out_ref[part, at, c * LANES : (c + 1) * LANES] = block.astype(BF16)

    columns_of(0)

    whole(ra.at[pl.ds(0, chips - 1)], 2).wait_recv()

    swap = remote(ra, rb, misc.at[2], misc.at[3], 2 * z + 1 - core)
    swap.start()
    swap.wait_recv()

    @pl.loop(0, chips)
    def _(i):
        own = pl.multiple_of(groups * (2 * i + core), groups)
        other = pl.multiple_of(groups * (2 * i + 1 - core), groups)
        tpad[pl.ds(HALF_WIDTH + own, groups), :] = ra[i].astype(F32)
        tpad[pl.ds(HALF_WIDTH + other, groups), :] = rb[i].astype(F32)

    series = groups * n
    tb[0] = tpad[HALF_WIDTH : 2 * HALF_WIDTH, :].astype(BF16)
    tb[1] = tpad[series : series + HALF_WIDTH, :].astype(BF16)
    aside = lax.rem(z + core + (1 - core) * (chips - 1), chips)
    edge = remote(tb.at[core], halo, misc.at[4], misc.at[5], 2 * aside + 1 - core)
    edge.start()
    for batch in range(2, len(BATCHES)):
        send_batch(batch)
    columns_of(1)
    edge.wait_recv()
    inside = ((z > 0) | (core == 1)) & ((z < chips - 1) | (core == 0))
    aside_rows = jnp.where(inside, halo[...].astype(F32), 0.0)
    edge_lane = iota((HALF_WIDTH, LANES), 1)
    above = jnp.where(edge_lane == 0, pltpu.roll(aside_rows, 1, 1), pltpu.roll(tpad[series : series + HALF_WIDTH, :], 1, 1))
    below = jnp.where(
        edge_lane == LANES - 1,
        pltpu.roll(aside_rows, LANES - 1, 1),
        pltpu.roll(tpad[HALF_WIDTH : 2 * HALF_WIDTH, :], LANES - 1, 1),
    )
    tpad[:HALF_WIDTH, :] = above
    tpad[series + HALF_WIDTH :, :] = below
    width = 2 * HALF_WIDTH

    @pl.loop(0, series // LANES)
    def _(i):
        at = pl.multiple_of(i * LANES, LANES)
        offset = iota((LANES, LANES + width), 1) - iota((LANES, LANES + width), 0)
        band = jnp.where((offset >= 0) & (offset <= width), 1.0, 0.0).astype(BF16)
        total = dot(band, tpad[pl.ds(at, LANES + width), :].astype(BF16))
        sm[:, pl.ds(at, LANES)] = total.T / (width + 1.0)

    own_rows = pl.ds(pl.multiple_of(core * rows, rows), rows)
    for i in range(series // LANES):
        smooth_ref[pl.ds(i, rows, stride=series // LANES), :] = sm[own_rows, i * LANES : (i + 1) * LANES]

    for batch in range(2, len(BATCHES)):
        columns_of(batch)

    whole(r1.at[others], 0).wait_send()
    whole(r2.at[others], 1).wait_send()
    whole(ra.at[pl.ds(0, chips - 1)], 2).wait_send()
    for batch in range(len(BATCHES)):
        whole(rows_of(batch), 3 + batch).wait_send()
    swap.wait_send()
    edge.wait_send()


def on_device(n, baseband, spectrum_in, dm_index):
    rows = spectrum_in.shape[1]
    chips = n // 2
    assert (rows * n, chips, n) == (ROW_LENGTH, ROWS_OUTER, COLS_OUTER)
    groups = LANES // DECIMATE_FACTOR
    blocks = baseband.reshape(2, rows, n, LANES).transpose(1, 2, 0, 3)
    matrices = (
        left_matrix(ROWS_OUTER, -1), left_matrix(ROWS_INNER, -1),
        left_matrix(COLS_OUTER, -1), right_matrix(COLS_INNER, -1),
        left_matrix(ROWS_OUTER, 1), left_matrix(ROWS_INNER, 1),
        left_matrix(COLS_OUTER, 1), right_matrix(COLS_INNER, 1),
    )
    block = pltpu.VMEM((n, 2 * rows, LANES), BF16)
    floats = pltpu.VMEM((n * 2 * rows, LANES), F32)
    dma = pltpu.SemaphoreType.DMA
    hbm = pl.BlockSpec(memory_space=pltpu.HBM)
    vmem = pl.BlockSpec(memory_space=pltpu.VMEM)
    spectrum_out, smoothed = pl.pallas_call(
        functools.partial(kernel, n, rows, "fft"),
        out_shape=(
            jax.ShapeDtypeStruct(spectrum_in.shape, BF16),
            jax.ShapeDtypeStruct((rows * groups * n // LANES, LANES), F32),
        ),
        in_specs=[pl.BlockSpec(memory_space=pltpu.SMEM)] + [hbm] * 10,
        out_specs=(vmem, vmem),
        scratch_shapes=[pltpu.VMEM(m.shape, BF16) for m in matrices] + [
            pltpu.VMEM(spectrum_in.shape, BF16), pltpu.VMEM((n, rows, 2, LANES), BF16), block, block, block, block, floats, floats,
            pltpu.VMEM((chips, groups, LANES), BF16), pltpu.VMEM((chips, groups, LANES), BF16),
            pltpu.VMEM((chips, groups, LANES), BF16), pltpu.VMEM((2, HALF_WIDTH, LANES), BF16),
            pltpu.VMEM((HALF_WIDTH, LANES), BF16), pltpu.VMEM((groups * n + 2 * HALF_WIDTH, LANES), F32),
            pltpu.VMEM((LANES, groups * n), F32),
            pltpu.VMEM((COLS_OUTER, LANES), F32), pltpu.VMEM((COLS_OUTER, LANES), F32),
            dma((3 + len(BATCHES),)), dma((3 + len(BATCHES),)), dma((6,)), dma((8,)),
            pltpu.SemaphoreType.REGULAR((int(math.log2(chips)) - 1,)),
        ],
        compiler_params=pltpu.CompilerParams(
            collective_id=0, has_side_effects=True, vmem_limit_bytes=36 * 2**20
        ),
        name="dedisperse",
    )(dm_index, *(pltpu.with_memory_space_constraint(a, pltpu.HBM) for a in (blocks, spectrum_in, *matrices)))
    return spectrum_out, smoothed.reshape(1, -1)


def solution(mesh):
    return jax.shard_map(
        functools.partial(on_device, mesh.shape["fft"]),
        mesh=mesh,
        in_specs=(P("beam", "fft"), P("beam", "fft", None), P()),
        out_specs=(P("beam", "fft", None), P("beam", "fft")),
        check_vma=False,
    )
```

```python
import functools
import math

import jax
import jax.numpy as jnp
import numpy as np
from jax import lax
from jax.experimental import pallas as pl
from jax.experimental.pallas import tpu as pltpu
from jax.sharding import PartitionSpec as P

ROWS_OUTER = 32
ROWS_INNER = 128
COLS_OUTER = 64
COLS_INNER = 128
ROW_LENGTH = 4096
COLUMN_LENGTH = 8192
SEGMENT_SAMPLES = 33554432
DM_GRID = 64
DECIMATE_FACTOR = 16
HALF_WIDTH = 16
LANES = 128
MESH = pl.DeviceIdType.MESH
BATCHES = ((0, 4), (4, 2), (6, 1), (7, 1))
F32 = jnp.float32
BF16 = jnp.bfloat16


def table(length, direction):
    product = np.outer(np.arange(length), np.arange(length)) % length
    radians = np.float32(direction * 2.0 * math.pi / length) * product.astype(np.float32)
    scale = np.float32(1.0 / math.sqrt(length))
    cosine = np.cos(radians).astype(np.float32) * scale
    sine = np.sin(radians).astype(np.float32) * scale
    return np.stack([np.stack([cosine, sine]), np.stack([-sine, cosine])])


def left_matrix(length, direction):
    return jnp.asarray(table(length, direction).transpose(1, 3, 0, 2).reshape(2 * length, 2 * length), BF16)


def right_matrix(length, direction):
    return jnp.asarray(table(length, direction).transpose(0, 2, 1, 3).reshape(2 * length, 2 * length), BF16)


def cos_sin(turns):
    quarter = jnp.round(turns * 4.0)
    theta = (turns - quarter * 0.25) * (2.0 * math.pi)
    z = theta * theta
    s = theta * (1.0 + z * (-1.0 / 6 + z * (1.0 / 120 + z * (-1.0 / 5040 + z * (1.0 / 362880)))))
    c = 1.0 + z * (-0.5 + z * (1.0 / 24 + z * (-1.0 / 720 + z * (1.0 / 40320))))
    q = quarter.astype(jnp.int32)
    odd = (q & 1) == 1
    cc = jnp.where(odd, s, c)
    ss = jnp.where(odd, c, s)
    cc = jnp.where(((q + 1) & 2) == 2, -cc, cc)
    ss = jnp.where((q & 2) == 2, -ss, ss)
    return cc, ss


def unit(numer, modulus):
    half = modulus // 2
    centred = ((numer + half) & (modulus - 1)) - half
    return cos_sin(centred.astype(F32) * (1.0 / modulus))


def iota(shape, dim):
    return lax.broadcasted_iota(jnp.int32, shape, dim)


def dot(a, b):
    return jnp.dot(a, b, preferred_element_type=F32)


def order(i, chips):
    t = chips - 1 - i
    odd = lax.rem(t, 2)
    return odd * lax.div(t + 1, 2) + (1 - odd) * (chips - lax.div(t, 2))


def columns(blocks, n, m3f, m4f, co, si, fa, fb):
    for d in range(n):
        fa[16 * d : 16 * (d + 1), :] = blocks(d).astype(F32)
    for m in range(8):
        x = jnp.concatenate([fa[pl.ds(8 * part + m, n, stride=16), :] for part in range(2)], axis=0)
        v = dot(m3f[...], x.astype(BF16))
        vr, vi = v[:COLS_OUTER], v[COLS_OUTER:]
        fb[pl.ds(m, COLS_OUTER, stride=8), :] = vr * co + vi * si
        fb[pl.ds(8 * COLS_OUTER + m, COLS_OUTER, stride=8), :] = vi * co - vr * si
    half = 8 * COLS_OUTER
    a = jnp.concatenate([fb[:half, :].astype(BF16), fb[half : 2 * half, :].astype(BF16)], axis=1)
    return dot(a, m4f[...])


def block_of(v, c, part):
    return v[8 * c : 8 * (c + 1), part * LANES : (part + 1) * LANES].astype(BF16)


def last_group(n, done, smooth, last, m3f, m4f, out, smooth_out, fa, fb, staged, sems):
    ready = BATCHES[-1][0] * 8
    copies = [
        pltpu.make_async_copy(done.at[:, pl.ds(0, ready)], out.at[:, pl.ds(0, ready)], sems.at[0]),
        pltpu.make_async_copy(smooth, smooth_out, sems.at[1]),
    ]
    for copy in copies:
        copy.start()
    co, si = unit(iota((COLS_OUTER, LANES), 0) * iota((COLS_OUTER, LANES), 1), COLUMN_LENGTH)
    v = columns(lambda d: last[16 * d : 16 * (d + 1), :], n, m3f, m4f, co, si, fa, fb)
    for c in range(COLS_OUTER):
        for part in range(2):
            staged[part, :, c * LANES : (c + 1) * LANES] = block_of(v, c, part)
    copies.append(pltpu.make_async_copy(staged, out.at[:, pl.ds(ready, 8)], sems.at[2]))
    copies[-1].start()
    for copy in copies:
        copy.wait()


def kernel(
    n, rows, axis,
    dm_ref, xb, spec, h1f, h2f, h3f, h4f, h1i, h2i, h3i, h4i,
    out_ref, smooth_ref, last, m3_out, m4_out,
    m1f, m2f, m3f, m4f, m1i, m2i, m3i, m4i, spec_v, r1, r2, r3, s2, s3, fa, fb, sd, ra, rb, tb, halo, tpad, sm, twc, tws,
    sent, got, misc, loaded, ready,
):
    me = lax.axis_index(axis)
    chips = n // 2
    z = lax.div(me, 2)
    core = lax.rem(me, 2)

    def peer(i):
        dz = order(lax.div(i, 2), chips)
        dc = 1 - lax.rem(i, 2)
        return lax.rem(z + dz, chips) * 2 + lax.rem(core + dc, 2)

    load_spec = pltpu.make_async_copy(spec, spec_v, misc.at[0])
    load_own = pltpu.make_async_copy(xb.at[:, me], r1.at[me], misc.at[1])
    pairs = zip((h1f, h2f, h3f, h4f, h1i, h2i, h3i, h4i), (m1f, m2f, m3f, m4f, m1i, m2i, m3i, m4i))
    loads = [load_spec] + [pltpu.make_async_copy(h, m, loaded.at[i]) for i, (h, m) in enumerate(pairs)]
    for load in loads:
        load.start()
    load_own.start()

    barrier = pltpu.get_barrier_semaphore()

    def within(reach):
        return 2 * max(chips - 1 - 2 * reach, 0)

    near = within(1)

    @pl.loop(near, n - 1)
    def _(i):
        pl.semaphore_signal(barrier, inc=1, device_id={axis: peer(i)}, device_id_type=MESH)

    pl.semaphore_wait(barrier, n - 1 - near)

    def remote(src, dst, send, recv, target):
        return pltpu.make_async_remote_copy(
            src_ref=src, dst_ref=dst, send_sem=send, recv_sem=recv,
            device_id={axis: target}, device_id_type=MESH,
        )

    def whole(ref, number):
        return remote(ref, ref, sent.at[number], got.at[number], 2 * z + 1 - core)

    others = pl.ds(0, n - 1)

    def rows_of(batch):
        first_group, count = BATCHES[batch]
        return r3.at[others, pl.ds(16 * first_group, 16 * count)]

    def first(i):
        x = peer(i)
        return remote(xb.at[:, x], r1.at[me], sent.at[0], got.at[0], x)

    def send_first(start, stop):
        @pl.loop(start, stop)
        def _(i):
            first(i).start()

    send_first(near, n - 1)
    for level in range(int(math.log2(chips)) - 1):
        reach = 2**level
        for side in (reach, chips - reach):
            target = 2 * lax.rem(z + side, chips) + core
            pl.semaphore_signal(ready.at[level], inc=1, device_id={axis: target}, device_id_type=MESH)
        pl.semaphore_wait(ready.at[level], 2)
        send_first(within(2 * reach), within(reach))

    m_iota = iota((rows, LANES), 0)
    lane = iota((rows, LANES), 1)
    freq_row = z + ROWS_OUTER * (rows * core + m_iota)
    steps = dm_ref[0] + 1
    row_turns = (steps * freq_row * freq_row).astype(F32) * (2.0 ** -33)
    for load in loads:
        load.wait()
    m3_out[...] = m3f[...]
    m4_out[...] = m4f[...]

    @pl.loop(0, COLS_OUTER)
    def _(c):
        at = pl.ds(pl.multiple_of(c * LANES, LANES), LANES)
        re = spec_v[0, :, at].astype(F32)
        im = spec_v[1, :, at].astype(F32)
        col = c + COLS_OUTER * lane
        cross = (steps * (freq_row * col)) & (2 * DM_GRID * COLUMN_LENGTH - 1)
        square = (steps * ((col * col) & 511)) & 511
        turns = row_turns + cross.astype(F32) * (0.5 / (DM_GRID * COLUMN_LENGTH)) + square.astype(F32) * (1.0 / 512)
        co, si = cos_sin(turns)
        a = jnp.concatenate([(re * co - im * si).astype(BF16), (re * si + im * co).astype(BF16)], axis=1)
        w = dot(a, m4i[...])
        wr, wi = w[:, :LANES], w[:, LANES:]
        co, si = unit(c * lane, COLUMN_LENGTH)
        fa[pl.ds(pl.multiple_of(c * rows, rows), rows), :] = wr * co - wi * si
        fa[pl.ds(pl.multiple_of((COLS_OUTER + c) * rows, rows), rows), :] = wr * si + wi * co

    half = iota((COLS_OUTER, LANES), 0)
    half_lane = iota((COLS_OUTER, LANES), 1)

    @pl.loop(0, rows)
    def _(m):
        x = fa[pl.ds(m, 2 * COLS_OUTER, stride=rows), :].astype(BF16)
        w = dot(m3i[...], x)
        wr, wi = w[:COLS_OUTER], w[COLS_OUTER:]
        k = z + ROWS_OUTER * (rows * core + m)
        co, si = unit((LANES * half + half_lane) * k, SEGMENT_SAMPLES)
        fb[pl.ds(m, COLS_OUTER, stride=2 * rows), :] = wr * co - wi * si
        fb[pl.ds(rows + m, COLS_OUTER, stride=2 * rows), :] = wr * si + wi * co

    def second(i):
        x = peer(i)
        return remote(s2.at[x], r2.at[me], sent.at[1], got.at[1], x)

    @pl.loop(0, n - 1)
    def _(i):
        x = peer(i)
        s2[x] = fb[pl.ds(pl.multiple_of(x * 2 * rows, 2 * rows), 2 * rows), :].astype(BF16)
        second(i).start()

    r2[me] = fb[pl.ds(pl.multiple_of(me * 2 * rows, 2 * rows), 2 * rows), :].astype(BF16)

    load_own.wait()

    whole(r1.at[others], 0).wait_recv()

    @pl.loop(0, n)
    def _(d):
        fa[pl.ds(pl.multiple_of(d * 2 * rows, 2 * rows), 2 * rows), :] = r1[d].astype(F32).reshape(2 * rows, LANES)

    p_iota = iota((ROWS_OUTER, LANES), 0)

    @pl.loop(0, rows)
    def _(j):
        def columns(g):
            start = g * 2 * rows + 2 * j
            parts = [fa[pl.ds(start + part, ROWS_OUTER, stride=4 * rows), :] for part in range(2)]
            return jnp.concatenate(parts, axis=0).astype(BF16)

        u = dot(m1f[...], jnp.concatenate([columns(0), columns(1)], axis=1))
        for g in range(2):
            n2 = g * rows + j
            ur = u[:ROWS_OUTER, g * LANES : (g + 1) * LANES]
            ui = u[ROWS_OUTER:, g * LANES : (g + 1) * LANES]
            co, si = unit(p_iota * n2, ROW_LENGTH)
            fb[pl.ds(n2, ROWS_OUTER, stride=ROWS_INNER), :] = ur * co + ui * si
            fb[pl.ds(ROW_LENGTH + n2, ROWS_OUTER, stride=ROWS_INNER), :] = ui * co - ur * si

    q_iota = iota((ROWS_INNER, LANES), 0)
    q_lane = iota((ROWS_INNER, LANES), 1)

    def third(batch, i):
        x = peer(i)
        first_group, count = BATCHES[batch]
        at = pl.ds(16 * first_group, 16 * count)
        return remote(s3.at[x, at], r3.at[me, at], sent.at[3 + batch], got.at[3 + batch], x)

    @pl.loop(0, chips)
    def _(i):
        p = lax.rem(z + order(i, chips), chips)
        at = pl.multiple_of(p * ROWS_INNER, ROWS_INNER)
        x = jnp.concatenate(
            [fb[pl.ds(at, ROWS_INNER), :].astype(BF16), fb[pl.ds(ROW_LENGTH + at, ROWS_INNER), :].astype(BF16)], axis=0
        )
        u = dot(m2f[...], x)
        ur, ui = u[:ROWS_INNER], u[ROWS_INNER:]
        co, si = unit((LANES * me + q_lane) * (p + ROWS_OUTER * q_iota), SEGMENT_SAMPLES)
        re = (ur * co + ui * si).reshape(2 * rows // 8, 1, 8, LANES)
        im = (ui * co - ur * si).reshape(2 * rows // 8, 1, 8, LANES)
        both = jnp.concatenate([re, im], axis=1).reshape(4 * rows, LANES).astype(BF16)
        s3[2 * p] = both[: 2 * rows]
        s3[2 * p + 1] = both[2 * rows :]
        third(0, 2 * i).start()

        @pl.when(i < chips - 1)
        def _():
            third(0, 2 * i + 1).start()

    r3[me] = s3[me]

    whole(r2.at[others], 1).wait_recv()

    @pl.loop(0, chips)
    def _(p):
        x = jnp.concatenate(
            [r2[2 * p, :rows, :], r2[2 * p + 1, :rows, :], r2[2 * p, rows:, :], r2[2 * p + 1, rows:, :]], axis=0
        )
        w = dot(m2i[...], x)
        wr, wi = w[:ROWS_INNER], w[ROWS_INNER:]
        co, si = unit(p * q_iota, ROW_LENGTH)
        at = pl.multiple_of(p * ROWS_INNER, ROWS_INNER)
        fa[pl.ds(at, ROWS_INNER), :] = wr * co - wi * si
        fa[pl.ds(ROW_LENGTH + at, ROWS_INNER), :] = wr * si + wi * co

    @pl.loop(0, rows)
    def _(j):
        x = jnp.concatenate(
            [fa[pl.ds(g * rows + j, 2 * ROWS_OUTER, stride=ROWS_INNER), :].astype(BF16) for g in range(2)], axis=1
        )
        w = dot(m1i[...], x).astype(BF16).astype(F32)
        power = w[:ROWS_OUTER] * w[:ROWS_OUTER] + w[ROWS_OUTER:] * w[ROWS_OUTER:]
        for g in range(2):
            fb[pl.ds(g * rows + j, ROWS_OUTER, stride=ROWS_INNER), :] = power[:, g * LANES : (g + 1) * LANES]

    groups = LANES // DECIMATE_FACTOR
    mean = (iota((groups, LANES), 1) // DECIMATE_FACTOR == iota((groups, LANES), 0)).astype(F32).astype(BF16)

    def averaged(at):
        power = fb[pl.ds(pl.multiple_of(at * ROWS_INNER, ROWS_INNER), ROWS_INNER), :]
        high = power.astype(BF16)
        low = (power - high.astype(F32)).astype(BF16)
        total = sum(
            lax.dot_general(mean, part, (((1,), (1,)), ((), ())), preferred_element_type=F32) for part in (high, low)
        )
        return (total * (1.0 / DECIMATE_FACTOR)).astype(BF16)

    def detected(i):
        x = lax.rem(z + order(i, chips), chips)
        return remote(sd.at[x], ra.at[z], sent.at[2], got.at[2], 2 * x + core)

    @pl.loop(0, chips - 1)
    def _(i):
        x = lax.rem(z + order(i, chips), chips)
        sd[x] = averaged(x)
        detected(i).start()

    def send_batch(batch):
        @pl.loop(0, n - 1)
        def _(i):
            third(batch, i).start()

    send_batch(1)
    ra[z] = averaged(z)

    co, si = unit(half * half_lane, COLUMN_LENGTH)
    twc[...] = co
    tws[...] = si

    def columns_of(batch):
        whole(rows_of(batch), 3 + batch).wait_recv()
        first_group, count = BATCHES[batch]

        @pl.loop(first_group, first_group + count)
        def _(g):
            at = pl.ds(pl.multiple_of(16 * g, 16), 16)
            v = columns(lambda d: r3[d, at, :], n, m3f, m4f, twc[...], tws[...], fa, fb)
            at = pl.ds(pl.multiple_of(8 * g, 8), 8)
            for c in range(COLS_OUTER):
                for part in range(2):
                    out_ref[part, at, c * LANES : (c + 1) * LANES] = block_of(v, c, part)

    columns_of(0)

    whole(ra.at[pl.ds(0, chips - 1)], 2).wait_recv()

    swap = remote(ra, rb, misc.at[2], misc.at[3], 2 * z + 1 - core)
    swap.start()
    swap.wait_recv()

    @pl.loop(0, chips)
    def _(i):
        own = pl.multiple_of(groups * (2 * i + core), groups)
        other = pl.multiple_of(groups * (2 * i + 1 - core), groups)
        tpad[pl.ds(HALF_WIDTH + own, groups), :] = ra[i].astype(F32)
        tpad[pl.ds(HALF_WIDTH + other, groups), :] = rb[i].astype(F32)

    series = groups * n
    tb[0] = tpad[HALF_WIDTH : 2 * HALF_WIDTH, :].astype(BF16)
    tb[1] = tpad[series : series + HALF_WIDTH, :].astype(BF16)
    aside = lax.rem(z + core + (1 - core) * (chips - 1), chips)
    edge = remote(tb.at[core], halo, misc.at[4], misc.at[5], 2 * aside + 1 - core)
    edge.start()
    for batch in range(2, len(BATCHES)):
        send_batch(batch)
    columns_of(1)
    edge.wait_recv()
    inside = ((z > 0) | (core == 1)) & ((z < chips - 1) | (core == 0))
    aside_rows = jnp.where(inside, halo[...].astype(F32), 0.0)
    edge_lane = iota((HALF_WIDTH, LANES), 1)
    above = jnp.where(edge_lane == 0, pltpu.roll(aside_rows, 1, 1), pltpu.roll(tpad[series : series + HALF_WIDTH, :], 1, 1))
    below = jnp.where(
        edge_lane == LANES - 1,
        pltpu.roll(aside_rows, LANES - 1, 1),
        pltpu.roll(tpad[HALF_WIDTH : 2 * HALF_WIDTH, :], LANES - 1, 1),
    )
    tpad[:HALF_WIDTH, :] = above
    tpad[series + HALF_WIDTH :, :] = below
    width = 2 * HALF_WIDTH

    @pl.loop(0, series // LANES)
    def _(i):
        at = pl.multiple_of(i * LANES, LANES)
        offset = iota((LANES, LANES + width), 1) - iota((LANES, LANES + width), 0)
        band = jnp.where((offset >= 0) & (offset <= width), 1.0, 0.0).astype(BF16)
        total = dot(band, tpad[pl.ds(at, LANES + width), :].astype(BF16))
        sm[:, pl.ds(at, LANES)] = total.T / (width + 1.0)

    own_rows = pl.ds(pl.multiple_of(core * rows, rows), rows)
    for i in range(series // LANES):
        smooth_ref[pl.ds(i, rows, stride=series // LANES), :] = sm[own_rows, i * LANES : (i + 1) * LANES]

    for batch in range(2, len(BATCHES) - 1):
        columns_of(batch)

    final = len(BATCHES) - 1
    whole(rows_of(final), 3 + final).wait_recv()
    for d in range(n):
        last[16 * d : 16 * (d + 1), :] = r3[d, 16 * BATCHES[final][0] : 16 * (BATCHES[final][0] + 1), :]


    whole(r1.at[others], 0).wait_send()
    whole(r2.at[others], 1).wait_send()
    whole(ra.at[pl.ds(0, chips - 1)], 2).wait_send()
    for batch in range(len(BATCHES)):
        whole(rows_of(batch), 3 + batch).wait_send()
    swap.wait_send()
    edge.wait_send()


def on_device(n, baseband, spectrum_in, dm_index):
    rows = spectrum_in.shape[1]
    chips = n // 2
    assert (rows * n, chips, n) == (ROW_LENGTH, ROWS_OUTER, COLS_OUTER)
    groups = LANES // DECIMATE_FACTOR
    blocks = baseband.reshape(2, rows, n, LANES).transpose(1, 2, 0, 3)
    matrices = (
        left_matrix(ROWS_OUTER, -1), left_matrix(ROWS_INNER, -1),
        left_matrix(COLS_OUTER, -1), right_matrix(COLS_INNER, -1),
        left_matrix(ROWS_OUTER, 1), left_matrix(ROWS_INNER, 1),
        left_matrix(COLS_OUTER, 1), right_matrix(COLS_INNER, 1),
    )
    block = pltpu.VMEM((n, 2 * rows, LANES), BF16)
    floats = pltpu.VMEM((n * 2 * rows, LANES), F32)
    dma = pltpu.SemaphoreType.DMA
    hbm = pl.BlockSpec(memory_space=pltpu.HBM)
    vmem = pl.BlockSpec(memory_space=pltpu.VMEM)
    parts = pl.pallas_call(
        functools.partial(kernel, n, rows, "fft"),
        out_shape=(
            jax.ShapeDtypeStruct(spectrum_in.shape, BF16),
            jax.ShapeDtypeStruct((rows * groups * n // LANES, LANES), F32),
            jax.ShapeDtypeStruct((16 * n, LANES), BF16),
            jax.ShapeDtypeStruct(matrices[2].shape, BF16),
            jax.ShapeDtypeStruct(matrices[3].shape, BF16),
        ),
        in_specs=[pl.BlockSpec(memory_space=pltpu.SMEM)] + [hbm] * 10,
        out_specs=(vmem,) * 5,
        scratch_shapes=[pltpu.VMEM(m.shape, BF16) for m in matrices] + [
            pltpu.VMEM(spectrum_in.shape, BF16), pltpu.VMEM((n, rows, 2, LANES), BF16), block, block, block, block, floats, floats,
            pltpu.VMEM((chips, groups, LANES), BF16), pltpu.VMEM((chips, groups, LANES), BF16),
            pltpu.VMEM((chips, groups, LANES), BF16), pltpu.VMEM((2, HALF_WIDTH, LANES), BF16),
            pltpu.VMEM((HALF_WIDTH, LANES), BF16), pltpu.VMEM((groups * n + 2 * HALF_WIDTH, LANES), F32),
            pltpu.VMEM((LANES, groups * n), F32),
            pltpu.VMEM((COLS_OUTER, LANES), F32), pltpu.VMEM((COLS_OUTER, LANES), F32),
            dma((3 + len(BATCHES),)), dma((3 + len(BATCHES),)), dma((6,)), dma((8,)),
            pltpu.SemaphoreType.REGULAR((int(math.log2(chips)) - 1,)),
        ],
        compiler_params=pltpu.CompilerParams(
            collective_id=0, has_side_effects=True, vmem_limit_bytes=36 * 2**20
        ),
        name="dedisperse",
    )(dm_index, *(pltpu.with_memory_space_constraint(a, pltpu.HBM) for a in (blocks, spectrum_in, *matrices)))
    floats = pltpu.VMEM((16 * n, LANES), F32)
    spectrum_out, smoothed = pl.pallas_call(
        functools.partial(last_group, n),
        out_shape=tuple(jax.ShapeDtypeStruct(a.shape, a.dtype) for a in parts[:2]),
        in_specs=[vmem] * 5,
        out_specs=(hbm, hbm),
        scratch_shapes=[floats, floats, pltpu.VMEM((2, 8, COLUMN_LENGTH), BF16), dma((3,))],
        name="last_group",
    )(*(pltpu.with_memory_space_constraint(a, pltpu.VMEM) for a in parts))
    return spectrum_out, smoothed.reshape(1, -1)


def solution(mesh):
    return jax.shard_map(
        functools.partial(on_device, mesh.shape["fft"]),
        mesh=mesh,
        in_specs=(P("beam", "fft"), P("beam", "fft", None), P()),
        out_specs=(P("beam", "fft", None), P("beam", "fft")),
        check_vma=False,
    )
```
